256 devices in a mesh: seq: 128 (over y, x_hi, z, core), fsdp: 2 (over x_lo).
Axes of the slice: x: 4 (x_hi: 2, x_lo: 2; x = x_hi * 2 + x_lo), y: 4, z: 8, core: 2. Of those that a mesh axis runs over, the one named last changes fastest.
Arguments:
- tokens: bfloat16 [512, 8192], P('seq', 'fsdp'), may hold values from -6 to 6
- gate_weight: bfloat16 [8192, 16384], P('fsdp', 'seq'), may hold values from -0.0625 to 0.0625
- up_weight: bfloat16 [8192, 16384], P('fsdp', 'seq'), may hold values from -0.0625 to 0.0625
- down_weight: bfloat16 [8192, 16384], P('fsdp', 'seq'), may hold values from -0.046875 to 0.046875
Outputs:
- mixed_out: bfloat16 [512, 8192], P('seq', 'fsdp')
The draws below stay inside these ranges and needn't reach their ends.
All inputs are finite; a program needn't handle non-finite values.
Results may differ from the reference program's by a relative error of at most 0.0049.
Values may be sent and summed in bfloat16 or wider, within the bound.
No kernel may reach another device: no remote copies, remote signals or barrier semaphores. Data moves between devices by JAX's collectives and lax.ppermute only.
A program may use at most 64 MiB of HBM per device.

```python
import jax
import jax.numpy as jnp
from jax import lax

D = 8192
FF = 16384
TOKENS = 512


def level_of(key, shape, split, low, top_value):
    def one(dim, parts):
        draws = jax.random.uniform(jax.random.fold_in(jax.random.fold_in(key, 6), dim), (parts,), jnp.float32, low / len(split), top_value / len(split))
        return jnp.repeat(jnp.exp(draws), shape[dim] // parts).reshape((-1,) + (1,) * (len(shape) - dim - 1))

    gain = one(*split[0])
    for cut in split[1:]:
        gain = gain * one(*cut)
    return gain


def scatter_about(rng, extent, spread, limit, shards=(), dtype=jnp.bfloat16):
    gain = level_of(rng, extent, shards, -0.22, 0.18) if shards else 1.0
    entries = jax.random.normal(rng, extent, jnp.float32) * spread * gain
    return jnp.minimum(jnp.maximum(entries, -limit), limit).astype(dtype)


def setup_inputs(seed: int = 0) -> dict:
    streams_of = jax.random.split(jax.random.key(seed), 5)
    return {
        "tokens": scatter_about(streams_of[0], (TOKENS, D), 1.0, 6.0, ((0, 128), (1, 2))),
        "gate_weight": scatter_about(streams_of[1], (D, FF), D ** -0.5, 0.0625, ((0, 2), (1, 128))),
        "up_weight": scatter_about(streams_of[2], (D, FF), D ** -0.5, 0.0625, ((0, 2), (1, 128))),
        "down_weight": scatter_about(streams_of[3], (D, FF), FF ** -0.5, 0.046875, ((0, 2), (1, 128))),
    }


def project_down(hidden, weight):
    return lax.dot_general(hidden, weight, (((1,), (1,)), ((), ())), preferred_element_type=jnp.float32)


def reference(tokens, gate_weight, up_weight, down_weight):
    gate_value = jnp.dot(tokens, gate_weight, preferred_element_type=jnp.float32)
    up_value = jnp.dot(tokens, up_weight, preferred_element_type=jnp.float32)
    hidden = (jax.nn.silu(gate_value) * up_value).astype(jnp.bfloat16)
    return project_down(hidden, down_weight).astype(jnp.bfloat16)
```

```python
import jax
import jax.numpy as jnp
from jax import lax
from jax.sharding import Mesh
from jax.sharding import PartitionSpec as P

AXES = ("y", "h", "z", "c")
PLANE = ("y", "h")
F32, BF16 = jnp.float32, jnp.bfloat16


def swapped(value, axis):
    return lax.ppermute(value, axis, [(0, 1), (1, 0)])


def shared(value, axes):
    copies = jnp.broadcast_to(value, (lax.axis_size(axes), *value.shape))
    return lax.all_to_all(copies, axes, 0, 0, tiled=True)


def summed(pieces, axes):
    arrived = lax.all_to_all(pieces, axes, 0, 0, tiled=True)
    return arrived.astype(F32).sum(axis=0)


def on_device(tokens, gate_weight, up_weight, down_weight):
    own, width = tokens.shape
    gates = jnp.concatenate([gate_weight, swapped(gate_weight, "c")], axis=1)
    ups = jnp.concatenate([up_weight, swapped(up_weight, "c")], axis=1)
    downs = jnp.concatenate([down_weight, swapped(down_weight, "c")], axis=1)
    line = shared(tokens, "z").reshape(-1, width)
    rows = shared(line, PLANE).reshape(-1, width)
    units = gates.shape[1]
    parts = jnp.dot(
        rows, jnp.concatenate([gates, ups], axis=1), preferred_element_type=F32
    )
    values = parts + swapped(parts.astype(BF16), "fsdp").astype(F32)
    hidden = (jax.nn.silu(values[:, :units]) * values[:, units:]).astype(BF16)
    out = lax.dot_general(
        hidden, downs, (((1,), (1,)), ((), ())), preferred_element_type=F32
    ).astype(BF16)
    mine = summed(out.reshape(-1, *line.shape), PLANE).astype(BF16)
    return summed(mine.reshape(-1, own, width), "z").astype(BF16)


def solution(mesh):
    finer = Mesh(
        mesh.devices.reshape(4, 2, 8, 2, mesh.shape["fsdp"]), (*AXES, "fsdp")
    )
    in_specs = (P(AXES, "fsdp"), P("fsdp", AXES), P("fsdp", AXES), P("fsdp", AXES))
    out_specs = P(AXES, "fsdp")
    return jax.shard_map(
        on_device, mesh=finer, in_specs=in_specs, out_specs=out_specs, check_vma=False
    )
```

```python
import jax
import jax.numpy as jnp
from jax import lax
from jax.sharding import Mesh
from jax.sharding import PartitionSpec as P

AXES = ("y", "h", "z", "c")
F32, BF16 = jnp.float32, jnp.bfloat16


def moved(value, axis, step):
    n = lax.axis_size(axis)
    return lax.ppermute(value, axis, [(i, (i + step) % n) for i in range(n)])


def shared(value, axis):
    copies = jnp.broadcast_to(value, (lax.axis_size(axis), *value.shape))
    return lax.all_to_all(copies, axis, 0, 0, tiled=True)


def plus(first, *others):
    total = first.astype(F32)
    for other in others:
        total = total + other.astype(F32)
    return total.astype(BF16)


def gathered_in_plane(own):
    half = own.shape[0] // 2
    top, bottom = own[:half], own[half:]
    before_top = moved(top, "y", 1)
    after_bottom = moved(bottom, "y", 3)
    before_bottom = moved(bottom, "y", 1)
    after_top = moved(top, "y", 3)
    other = moved(own, "h", 1)
    far_top = moved(before_top, "y", 1)
    far_bottom = moved(after_bottom, "y", 3)
    before_other = moved(other, "y", 1)
    after_other = moved(other, "y", 3)
    far = jnp.concatenate([far_top, far_bottom], axis=0)
    far_other = moved(far, "h", 1)
    return [
        own, before_top, before_bottom, after_top, after_bottom, far,
        other, before_other, after_other, far_other,
    ]


def summed_in_plane(out, rows):
    half = rows // 2

    def block(i, part=None):
        start = i * rows
        if part is None:
            return out[start : start + rows]
        return out[start + part * half : start + (part + 1) * half]

    own, before, after, far, other, before_other, after_other, far_other = range(8)
    far_in = moved(block(far_other), "h", 1)
    from_after = moved(block(before_other), "y", 3)
    from_before = moved(block(after_other), "y", 1)
    far_top = plus(block(far, 0), far_in[:half])
    far_bottom = plus(block(far, 1), far_in[half:])
    relay_top = moved(far_top, "y", 3)
    relay_bottom = moved(far_bottom, "y", 1)
    other_in = moved(plus(block(other), from_after, from_before), "h", 1)
    after_bottom = moved(block(before, 1), "y", 3)
    before_top = moved(block(after, 0), "y", 1)
    after_top = moved(plus(block(before, 0), relay_top), "y", 3)
    before_bottom = moved(plus(block(after, 1), relay_bottom), "y", 1)
    top = plus(block(own, 0), after_top, before_top, other_in[:half])
    bottom = plus(block(own, 1), after_bottom, before_bottom, other_in[half:])
    return jnp.concatenate([top, bottom], axis=0)


def on_device(tokens, gate_weight, up_weight, down_weight):
    count, width = tokens.shape
    gates = jnp.concatenate([gate_weight, moved(gate_weight, "c", 1)], axis=1)
    ups = jnp.concatenate([up_weight, moved(up_weight, "c", 1)], axis=1)
    downs = jnp.concatenate([down_weight, moved(down_weight, "c", 1)], axis=1)
    line = shared(tokens, "z").reshape(-1, width)
    rows = jnp.concatenate(gathered_in_plane(line), axis=0)
    units = gates.shape[1]
    parts = jnp.dot(
        rows, jnp.concatenate([gates, ups], axis=1), preferred_element_type=F32
    )
    values = parts + moved(parts.astype(BF16), "fsdp", 1).astype(F32)
    hidden = (jax.nn.silu(values[:, :units]) * values[:, units:]).astype(BF16)
    out = lax.dot_general(
        hidden, downs, (((1,), (1,)), ((), ())), preferred_element_type=F32
    ).astype(BF16)
    mine = summed_in_plane(out, line.shape[0])
    pieces = lax.all_to_all(
        mine.reshape(-1, count, width), "z", 0, 0, tiled=True
    )
    return plus(*pieces)


def solution(mesh):
    finer = Mesh(
        mesh.devices.reshape(4, 2, 8, 2, mesh.shape["fsdp"]), (*AXES, "fsdp")
    )
    in_specs = (P(AXES, "fsdp"), P("fsdp", AXES), P("fsdp", AXES), P("fsdp", AXES))
    out_specs = P(AXES, "fsdp")
    return jax.shard_map(
        on_device, mesh=finer, in_specs=in_specs, out_specs=out_specs, check_vma=False
    )
```

```python
import jax
import jax.numpy as jnp
from jax import lax
from jax.experimental import pallas as pl
from jax.experimental.pallas import tpu as pltpu
from jax.sharding import Mesh
from jax.sharding import PartitionSpec as P


AXES = ("y", "h", "z", "c")
F32, BF16 = jnp.float32, jnp.bfloat16
STEP = 512
VMEM_LIMIT = 16 * 2**20


def moved(value, axis, step):
    n = lax.axis_size(axis)
    return lax.ppermute(value, axis, [(i, (i + step) % n) for i in range(n)])


def shared(value, axis):
    copies = jnp.broadcast_to(value, (lax.axis_size(axis), *value.shape))
    return lax.all_to_all(copies, axis, 0, 0, tiled=True)


def gathered_in_plane(own):
    before = moved(own, "y", 1)
    after = moved(own, "y", 3)
    other = moved(own, "h", 1)
    far = [moved(halves(before)[0], "y", 1), moved(halves(after)[1], "y", 3)]
    far = jnp.concatenate(far, axis=0)
    b_other = moved(other, "y", 1)
    a_other = moved(other, "y", 3)
    far_other = moved(far, "h", 1)
    return (own, before, after, other), (far, b_other, a_other, far_other)


def plus(first, *others):
    total = first.astype(F32)
    for other in others:
        total = total + other.astype(F32)
    return total.astype(BF16)


def halves(value):
    half = value.shape[0] // 2
    return value[:half], value[half:]


def on_core(kernel, outs, flops, *args):
    vmem = pl.BlockSpec(memory_space=pltpu.VMEM)
    moved_bytes = sum(a.size * a.dtype.itemsize for a in (*args, *outs))
    return pl.pallas_call(
        kernel,
        out_shape=outs,
        in_specs=[vmem] * len(args),
        out_specs=[vmem] * len(outs),
        compiler_params=pltpu.CompilerParams(vmem_limit_bytes=VMEM_LIMIT),
        cost_estimate=pl.CostEstimate(
            flops=flops, transcendentals=0, bytes_accessed=moved_bytes
        ),
    )(*args)


def parts_of(blocks, gates, ups):
    depth, half = gates[0].shape
    rows = sum(b.shape[0] for b in blocks)

    def kernel(*refs):
        *block_refs, g0, g1, u0, u1, out = refs
        for pair, at in (((g0, g1), 0), ((u0, u1), 2 * half)):
            total = jnp.zeros((rows, 2 * half), F32)
            for k in range(0, depth, STEP):
                cut = (slice(None), pl.ds(k, STEP))
                left = jnp.concatenate([b[cut] for b in block_refs], axis=0)
                cut = (pl.ds(k, STEP), slice(None))
                right = jnp.concatenate([w[cut] for w in pair], axis=1)
                total += jnp.dot(left, right, preferred_element_type=F32)
            out[:, at : at + 2 * half] = total

    outs = [jax.ShapeDtypeStruct((rows, 4 * half), F32)]
    flops = 8 * rows * depth * half
    return on_core(kernel, outs, flops, *blocks, *gates, *ups)[0]


def projected(parts, came, downs, sizes):
    width, half = downs[0].shape

    def kernel(parts, came, d0, d1, *outs):
        values = parts[...] + came[...].astype(F32)
        gate, up = values[:, : 2 * half], values[:, 2 * half :]
        hidden = (gate / (1 + jnp.exp(-gate)) * up).astype(BF16)
        for n in range(0, width, STEP):
            cut = (pl.ds(n, STEP), slice(None))
            right = jnp.concatenate([d0[cut], d1[cut]], axis=1)
            out = lax.dot_general(
                hidden, right, (((1,), (1,)), ((), ())), preferred_element_type=F32
            ).astype(BF16)
            at = 0
            for size, ref in zip(sizes, outs):
                ref[:, n : n + STEP] = out[at : at + size]
                at += size

    outs = [jax.ShapeDtypeStruct((size, width), BF16) for size in sizes]
    flops = 4 * sum(sizes) * width * half
    return on_core(kernel, outs, flops, parts, came, *downs)


def summed_in_plane(near, away):
    own, before, after, other = near
    far, b_other, a_other, far_other = away
    far = plus(far, moved(far_other, "h", 1))
    from_after_o = moved(b_other, "y", 3)
    from_before_o = moved(a_other, "y", 1)
    top, bottom = halves(far)
    top = moved(top, "y", 3)
    bottom = moved(bottom, "y", 1)
    before_top, before_bottom = halves(before)
    after_top, after_bottom = halves(after)
    early_top = moved(after_top, "y", 1)
    early_bottom = moved(before_bottom, "y", 3)
    from_other = moved(plus(other, from_after_o, from_before_o), "h", 1)
    late_top = moved(plus(before_top, top), "y", 3)
    late_bottom = moved(plus(after_bottom, bottom), "y", 1)
    early = jnp.concatenate([early_top, early_bottom], axis=0)
    late = jnp.concatenate([late_top, late_bottom], axis=0)
    return plus(own, early, late, from_other)


def on_device(tokens, gate_weight, up_weight, down_weight):
    count, width = tokens.shape
    gates = gate_weight, moved(gate_weight, "c", 1)
    ups = up_weight, moved(up_weight, "c", 1)
    downs = down_weight, moved(down_weight, "c", 1)
    own = shared(tokens, "z").reshape(-1, width)
    near, away = gathered_in_plane(own)
    near = parts_of(near, gates, ups)
    away = parts_of(away, gates, ups)
    near_in = moved(near, "fsdp", 1)
    away_in = moved(away.astype(BF16), "fsdp", 1)
    sizes = (own.shape[0],) * 4
    away = projected(away, away_in, downs, sizes)
    near = projected(near, near_in, downs, sizes)
    mine = summed_in_plane(near, away)
    pieces = mine.reshape(-1, count, width)
    arrived = lax.all_to_all(pieces, "z", 0, 0, tiled=True)
    return plus(*arrived)


def solution(mesh):
    finer = Mesh(
        mesh.devices.reshape(4, 2, 8, 2, mesh.shape["fsdp"]), (*AXES, "fsdp")
    )
    in_specs = (P(AXES, "fsdp"), P("fsdp", AXES), P("fsdp", AXES), P("fsdp", AXES))
    out_specs = P(AXES, "fsdp")

    return jax.shard_map(
        on_device, mesh=finer, in_specs=in_specs, out_specs=out_specs, check_vma=False
    )
```

```python
import jax
import jax.numpy as jnp
from jax import lax
from jax.experimental import pallas as pl
from jax.experimental.pallas import tpu as pltpu
from jax.sharding import Mesh
from jax.sharding import PartitionSpec as P


AXES = ("y", "h", "z", "c")
F32, BF16 = jnp.float32, jnp.bfloat16
STEP = 512
VMEM_LIMIT = 16 * 2**20


def moved(value, axis, step):
    n = lax.axis_size(axis)
    return lax.ppermute(value, axis, [(i, (i + step) % n) for i in range(n)])


def shared(value, axis):
    copies = jnp.broadcast_to(value, (lax.axis_size(axis), *value.shape))
    return lax.all_to_all(copies, axis, 0, 0, tiled=True)


def gathered_in_plane(own):
    before = moved(own, "y", 1)
    after = moved(own, "y", 3)
    other = moved(own, "h", 1)
    far = [moved(halves(before)[0], "y", 1), moved(halves(after)[1], "y", 3)]
    far = jnp.concatenate(far, axis=0)
    b_other = moved(other, "y", 1)
    a_other = moved(other, "y", 3)
    far_other = moved(far, "h", 1)
    return (own, before, after), (other, far, b_other, a_other, far_other)


def plus(first, *others):
    total = first.astype(F32)
    for other in others:
        total = total + other.astype(F32)
    return total.astype(BF16)


def halves(value):
    half = value.shape[0] // 2
    return value[:half], value[half:]


def on_core(kernel, outs, flops, *args):
    vmem = pl.BlockSpec(memory_space=pltpu.VMEM)
    moved_bytes = sum(a.size * a.dtype.itemsize for a in (*args, *outs))
    return pl.pallas_call(
        kernel,
        out_shape=outs,
        in_specs=[vmem] * len(args),
        out_specs=[vmem] * len(outs),
        compiler_params=pltpu.CompilerParams(vmem_limit_bytes=VMEM_LIMIT),
        cost_estimate=pl.CostEstimate(
            flops=flops, transcendentals=0, bytes_accessed=moved_bytes
        ),
    )(*args)


def parts_of(blocks, gates, ups, kinds):
    depth, half = gates[0].shape
    rows = sum(b.shape[0] for b in blocks)

    def kernel(*refs):
        block_refs, weights = refs[: len(blocks)], refs[len(blocks) :]
        g0, g1, u0, u1, *outs = weights
        for pair, at in (((g0, g1), 0), ((u0, u1), 2 * half)):
            total = jnp.zeros((rows, 2 * half), F32)
            for k in range(0, depth, STEP):
                cut = (slice(None), pl.ds(k, STEP))
                left = jnp.concatenate([b[cut] for b in block_refs], axis=0)
                cut = (pl.ds(k, STEP), slice(None))
                right = jnp.concatenate([w[cut] for w in pair], axis=1)
                total += jnp.dot(left, right, preferred_element_type=F32)
            for out in outs:
                out[:, at : at + 2 * half] = total.astype(out.dtype)

    outs = [jax.ShapeDtypeStruct((rows, 4 * half), kind) for kind in kinds]
    flops = 8 * rows * depth * half
    return on_core(kernel, outs, flops, *blocks, *gates, *ups)


def projected(parts, came, downs, pieces):
    width, half = downs[0].shape

    def kernel(parts, came, d0, d1, *outs):
        values = parts[...] + came[...].astype(F32)
        gate, up = values[:, : 2 * half], values[:, 2 * half :]
        hidden = (gate / (1 + jnp.exp(-gate)) * up).astype(BF16)
        for n in range(0, width, STEP):
            cut = slice(n, n + STEP)
            right = jnp.concatenate([d0[cut], d1[cut]], axis=1)
            out = lax.dot_general(
                hidden, right, (((1,), (1,)), ((), ())), preferred_element_type=F32
            ).astype(BF16)
            at = 0
            for rows, ref in zip(pieces, outs):
                ref[:, cut] = out[at : at + rows]
                at += rows

    outs = [jax.ShapeDtypeStruct((rows, width), BF16) for rows in pieces]
    flops = 4 * parts.shape[0] * width * half
    return on_core(kernel, outs, flops, parts, came, *downs)


def summed_in_plane(near, away):
    own, before_top, before_bottom, after_top, after_bottom = near
    other, far, b_other, a_other, far_other = away
    far = plus(far, moved(far_other, "h", 1))
    from_after = moved(b_other, "y", 3)
    from_before = moved(a_other, "y", 1)
    top, bottom = halves(far)
    top = moved(top, "y", 3)
    bottom = moved(bottom, "y", 1)
    early_top = moved(after_top, "y", 1)
    early_bottom = moved(before_bottom, "y", 3)
    from_other = moved(plus(other, from_after, from_before), "h", 1)
    late_top = moved(plus(before_top, top), "y", 3)
    late_bottom = moved(plus(after_bottom, bottom), "y", 1)
    own_top, own_bottom = halves(own)
    other_top, other_bottom = halves(from_other)
    top = plus(own_top, early_top, late_top, other_top)
    bottom = plus(own_bottom, early_bottom, late_bottom, other_bottom)
    return jnp.concatenate([top, bottom], axis=0)


def on_device(tokens, gate_weight, up_weight, down_weight):
    count, width = tokens.shape
    gates = gate_weight, moved(gate_weight, "c", 1)
    ups = up_weight, moved(up_weight, "c", 1)
    downs = down_weight, moved(down_weight, "c", 1)
    own = shared(tokens, "z").reshape(-1, width)
    near, away = gathered_in_plane(own)
    (near,) = parts_of(near, gates, ups, (F32,))
    near_in = moved(near, "fsdp", 1)
    away, sent = parts_of(away, gates, ups, (F32, BF16))
    away_in = moved(sent, "fsdp", 1)
    n = own.shape[0]
    half = n // 2
    near = projected(near, near_in, downs, (n, half, half, half, half))
    away = projected(away, away_in, downs, (n,) * 5)
    mine = summed_in_plane(near, away)
    pieces = mine.reshape(-1, count, width)
    arrived = lax.all_to_all(pieces, "z", 0, 0, tiled=True)
    return plus(*arrived)


def solution(mesh):
    finer = Mesh(
        mesh.devices.reshape(4, 2, 8, 2, mesh.shape["fsdp"]), (*AXES, "fsdp")
    )
    in_specs = (P(AXES, "fsdp"), P("fsdp", AXES), P("fsdp", AXES), P("fsdp", AXES))
    out_specs = P(AXES, "fsdp")

    return jax.shard_map(
        on_device, mesh=finer, in_specs=in_specs, out_specs=out_specs, check_vma=False
    )
```

```python
import jax
import jax.numpy as jnp
from jax import lax
from jax.experimental import pallas as pl
from jax.experimental.pallas import tpu as pltpu
from jax.sharding import Mesh
from jax.sharding import PartitionSpec as P


AXES = ("y", "h", "z", "c")
F32, BF16 = jnp.float32, jnp.bfloat16
STEP = 512
VMEM_LIMIT = 16 * 2**20


def moved(value, axis, step):
    n = lax.axis_size(axis)
    return lax.ppermute(value, axis, [(i, (i + step) % n) for i in range(n)])


def shared(value, axis):
    copies = jnp.broadcast_to(value, (lax.axis_size(axis), *value.shape))
    return lax.all_to_all(copies, axis, 0, 0, tiled=True)


def gathered_in_plane(own):
    far = moved(own, "y", 2)
    other = moved(own, "h", 1)
    before = moved(own, "y", 1)
    after = moved(own, "y", 3)
    b_other = moved(other, "y", 1)
    a_other = moved(other, "y", 3)
    far_other = moved(far, "h", 1)
    return (own, before, after), (other, far), (b_other, a_other, far_other)


def plus(first, *others):
    total = first.astype(F32)
    for other in others:
        total = total + other.astype(F32)
    return total.astype(BF16)


def on_core(kernel, outs, flops, *args):
    vmem = pl.BlockSpec(memory_space=pltpu.VMEM)
    moved_bytes = sum(a.size * a.dtype.itemsize for a in (*args, *outs))
    return pl.pallas_call(
        kernel,
        out_shape=outs,
        in_specs=[vmem] * len(args),
        out_specs=[vmem] * len(outs),
        compiler_params=pltpu.CompilerParams(vmem_limit_bytes=VMEM_LIMIT),
        cost_estimate=pl.CostEstimate(
            flops=flops, transcendentals=0, bytes_accessed=moved_bytes
        ),
    )(*args)


def held(value):
    def kernel(source, out, sem):
        copy = pltpu.make_async_copy(source, out, sem)
        copy.start()
        copy.wait()

    return pl.pallas_call(
        kernel,
        out_shape=jax.ShapeDtypeStruct(value.shape, value.dtype),
        in_specs=[pl.BlockSpec(memory_space=pl.ANY)],
        out_specs=pl.BlockSpec(memory_space=pltpu.VMEM),
        scratch_shapes=[pltpu.SemaphoreType.DMA],
        compiler_params=pltpu.CompilerParams(vmem_limit_bytes=VMEM_LIMIT),
    )(value)


def parts_of(blocks, gates, ups, kinds):
    depth, half = gates[0].shape
    rows = sum(b.shape[0] for b in blocks)

    def kernel(*refs):
        block_refs, weights = refs[: len(blocks)], refs[len(blocks) :]
        g0, g1, u0, u1, *outs = weights
        for pair, at in (((g0, g1), 0), ((u0, u1), 2 * half)):
            total = jnp.zeros((rows, 2 * half), F32)
            for k in range(0, depth, STEP):
                cut = (slice(None), pl.ds(k, STEP))
                left = jnp.concatenate([b[cut] for b in block_refs], axis=0)
                cut = (pl.ds(k, STEP), slice(None))
                right = jnp.concatenate([w[cut] for w in pair], axis=1)
                total += jnp.dot(left, right, preferred_element_type=F32)
            for out in outs:
                out[:, at : at + 2 * half] = total.astype(out.dtype)

    outs = [jax.ShapeDtypeStruct((rows, 4 * half), kind) for kind in kinds]
    flops = 8 * rows * depth * half
    return on_core(kernel, outs, flops, *blocks, *gates, *ups)


def projected(parts, came, downs, pieces):
    width, half = downs[0].shape

    def kernel(parts, came, d0, d1, *outs):
        values = parts[...] + came[...].astype(F32)
        gate, up = values[:, : 2 * half], values[:, 2 * half :]
        hidden = (gate / (1 + jnp.exp(-gate)) * up).astype(BF16)
        for n in range(0, width, STEP):
            cut = slice(n, n + STEP)
            right = jnp.concatenate([d0[cut], d1[cut]], axis=1)
            out = lax.dot_general(
                hidden, right, (((1,), (1,)), ((), ())), preferred_element_type=F32
            ).astype(BF16)
            at = 0
            for rows, ref in zip(pieces, outs):
                ref[:, cut] = out[at : at + rows]
                at += rows

    outs = [jax.ShapeDtypeStruct((rows, width), BF16) for rows in pieces]
    flops = 4 * parts.shape[0] * width * half
    return on_core(kernel, outs, flops, parts, came, *downs)


def summed_in_plane(near, mid, away):
    own, before, after = near
    other, far = mid
    b_other, a_other, far_other = away
    far = plus(far, moved(far_other, "h", 1))
    from_after = moved(b_other, "y", 3)
    from_before = moved(a_other, "y", 1)
    other = plus(other, from_after, from_before)
    from_after = moved(before, "y", 3)
    from_before = moved(after, "y", 1)
    from_far = moved(far, "y", 2)
    from_other = moved(other, "h", 1)
    return plus(own, from_after, from_before, from_far, from_other)


def on_device(tokens, gate_weight, up_weight, down_weight):
    count, width = tokens.shape
    up_weight = held(up_weight)
    gates = gate_weight, moved(gate_weight, "c", 1)
    ups = up_weight, moved(up_weight, "c", 1)
    downs = down_weight, moved(down_weight, "c", 1)
    own = shared(tokens, "z").reshape(-1, width)
    near, mid, away = gathered_in_plane(own)
    (near,) = parts_of(near, gates, ups, (F32,))
    near_in = moved(near, "fsdp", 1)
    (mid,) = parts_of(mid, gates, ups, (F32,))
    mid_in = moved(mid, "fsdp", 1)
    away, sent = parts_of(away, gates, ups, (F32, BF16))
    away_in = moved(sent, "fsdp", 1)
    n = own.shape[0]
    near = projected(near, near_in, downs, (n,) * 3)
    mid = projected(mid, mid_in, downs, (n, n))
    away = projected(away, away_in, downs, (n,) * 3)
    mine = summed_in_plane(near, mid, away)
    pieces = mine.reshape(-1, count, width)
    arrived = lax.all_to_all(pieces, "z", 0, 0, tiled=True)
    return plus(*arrived)


def solution(mesh):
    finer = Mesh(
        mesh.devices.reshape(4, 2, 8, 2, mesh.shape["fsdp"]), (*AXES, "fsdp")
    )
    in_specs = (P(AXES, "fsdp"), P("fsdp", AXES), P("fsdp", AXES), P("fsdp", AXES))
    out_specs = P(AXES, "fsdp")

    return jax.shard_map(
        on_device, mesh=finer, in_specs=in_specs, out_specs=out_specs, check_vma=False
    )
```
